32 devices in a mesh: basin: 2 (over x), recv: 8 (over z, y), src: 2 (over core).
Axes of the slice: x: 2, y: 2, z: 4, core: 2. Of those that a mesh axis runs over, the one named last changes fastest.
Arguments:
- positions: float32 [3, 4096], P(None, ('basin', 'recv', 'src')), parts along dimension 1, may hold values from -1.1 to 1.1, as said below
- normals: float32 [3, 4096], P(None, ('basin', 'recv', 'src')), parts along dimension 1, may hold values from -1 to 1, as said below
- area: float32 [4096], P(('basin', 'recv', 'src')), parts along dimension 0, may hold values from 0.0009765625 to 0.0078125
- albedo: float32 [4096], P(('basin', 'recv', 'src')), parts along dimension 0, may hold values from 0.1 to 0.6
- conductivity: float32 [4096], P(('basin', 'recv', 'src')), parts along dimension 0, may hold values from 0.05 to 0.4
- soil: float32 [32, 4096], P(None, ('basin', 'recv', 'src')), parts along dimension 1, may hold values from 0.5 to 1.2
- sun_tan: float32 [16], replicated, may hold values from 0.05 to 2
- samples: int32 [32, 32], P(('basin', 'recv', 'src')), parts along dimension 0, may hold values from 1 to 2047
- occupancy: int32 [32, 16], P('basin'), parts along dimension 0, may hold values 0 or 1
Outputs:
- soil_final: float32 [32, 4096], P(None, ('basin', 'recv', 'src')), parts along dimension 1
- bounce: float32 [16, 4096], P(None, ('basin', 'recv', 'src')), parts along dimension 1
The draws below stay inside these ranges and needn't reach their ends.
There are 2 independent parts, one for each index of `basin`. The reference program is written for one: setup_inputs(seed, part) draws one part's arguments, and reference() takes and returns one part's arrays. A program takes and returns all parts, laid end to end along the dimension named above; an argument that names none is the same for every part. Nothing has to cross between parts.
Inputs may be any that keep to these rules, and one draw needn't show every extreme that they name: `positions`: facets lie on a bowl below z = 0. `normals`: each column has unit length.
All inputs are finite; a program needn't handle non-finite values.
Results may differ from the reference program's by a relative error of at most 0.0003.
Values may be sent and summed in bfloat16 or wider, within the bound.
A program may use at most 64 MiB of HBM per device.

```python
import math
import jax
import jax.numpy as jnp
from jax import lax

FAC = 128
SAMPLES = 32
LAYERS = 32
F = 2048
AZIMUTHS = 16
EPOCHS = 16
BLOCKS = 16


def bowl_shape(key):
    base = jax.random.fold_in(key, 31)
    first, second, third, fourth_key = jax.random.split(base, 4)
    turn = jax.random.uniform(first, (F,), jnp.float32, 0.0, 2.0 * math.pi)
    depth = jax.random.uniform(second, (F,), jnp.float32, 0.0, 1.0)
    radius = jax.random.uniform(third, (F,), jnp.float32, 0.9, 1.1)
    side = jnp.sqrt(1.0 - depth * depth)
    unit = jnp.stack([side * jnp.cos(turn), side * jnp.sin(turn), -depth])
    jitter = jax.random.uniform(fourth_key, (3, F), jnp.float32, -0.3, 0.3)
    facing = jitter - unit
    facing = facing / jnp.sqrt(jnp.sum(facing * facing, axis=0, keepdims=True))
    return (radius[None, :] * unit, facing)


def draw_positions(key, part):
    return bowl_shape(key)[0]


def draw_normals(key, part):
    return bowl_shape(key)[1]


def touch_ends(result, own_key, smallest, top_value):
    extent = result.shape
    index_at = [jax.random.randint(jax.random.fold_in(own_key, axis), (), 0, extent[axis]) for axis in range(len(extent))]
    result = result.at[tuple(index_at)].set(smallest)
    longest = extent.index(max(extent))
    index_at[longest] = (index_at[longest] + 1) % extent[longest]
    return result.at[tuple(index_at)].set(top_value)


def shard_levels(own_key, shape, cuts, smallest, top_value):
    loudness = 1.0
    for dim, blocks in cuts:
        steps = jax.random.uniform(jax.random.fold_in(jax.random.fold_in(own_key, 6), dim), (blocks,), jnp.float32, smallest / len(cuts), top_value / len(cuts))
        loudness = loudness * jnp.repeat(jnp.exp(steps), shape[dim] // blocks).reshape((-1,) + (1,) * (len(shape) - 1 - dim))
    return loudness


def setup_inputs(seed: int = 0, part: int = 0) -> dict:
    arg_keys = jax.random.split(jax.random.key(seed), 10)
    own_keys = jax.random.split(jax.random.fold_in(arg_keys[9], part), 10)
    return {
        "positions": draw_positions(jax.random.fold_in(jax.random.fold_in(arg_keys[9], part), 71), part),
        "normals": draw_normals(jax.random.fold_in(jax.random.fold_in(arg_keys[9], part), 71), part),
        "area": jnp.clip(jnp.exp(math.log(0.0078125) - 2.0794415 * jax.random.uniform(own_keys[2], (F,), jnp.float32) ** shard_levels(own_keys[2], (F,), ((0, 16),), -0.2, 0.2)), 0.0009765625, 0.0078125),
        "albedo": jnp.clip(0.1 + 0.5 * jax.random.uniform(own_keys[3], (F,), jnp.float32) ** shard_levels(own_keys[3], (F,), ((0, 16),), -0.2, 0.2), 0.1, 0.6),
        "conductivity": jnp.clip(jnp.exp(math.log(0.4) - 2.0794415 * jax.random.uniform(own_keys[4], (F,), jnp.float32) ** shard_levels(own_keys[4], (F,), ((0, 16),), -0.2, 0.2)), 0.05, 0.4),
        "soil": jnp.clip(0.5 + 0.70000005 * jax.random.uniform(own_keys[5], (LAYERS, F), jnp.float32) ** shard_levels(own_keys[5], (LAYERS, F), ((1, 16),), -0.2, 0.2), 0.5, 1.2),
        "sun_tan": jnp.clip(jax.random.uniform(arg_keys[6], (EPOCHS,), jnp.float32, 0.05, 2.0), 0.05, 2.0),
        "samples": touch_ends(jax.random.randint(own_keys[7], (AZIMUTHS, SAMPLES), 1, min(F, 4096)), jax.random.fold_in(own_keys[7], 1), 1, (min(F, 4096)) - 1).astype(jnp.int32),
        "occupancy": touch_ends((jax.random.randint(own_keys[8], (BLOCKS, BLOCKS), 0, 3) < 2).astype(jnp.int32), jax.random.fold_in(own_keys[8], 1), 0, 1),
    }


solar_flux = 2.0
emissivity = 0.9
surface_gain = 0.1
shade_width = 0.1
reach_offset = 0.05

def fourth(value):
    square = value * value
    return square * square

def rotate(values, shift):
    count = values.shape[0]
    doubled = jnp.concatenate([values, values], 0)
    return lax.dynamic_slice_in_dim(doubled, shift.astype(jnp.int32), count, 0)

def profile_max(coords, offsets):
    px, py, pz = (coords[0], coords[1], coords[2])
    count = px.shape[0]

    def sweep(best, shift):
        delta_x = rotate(px, shift) - px
        delta_y = rotate(py, shift) - py
        reach = jnp.sqrt(delta_x * delta_x + delta_y * delta_y) + reach_offset
        slope = (rotate(pz, shift) - pz) / reach
        return (jnp.maximum(best, slope), None)
    start = jnp.full((count,), -1e+30, jnp.float32)
    best, unused = lax.scan(sweep, start, offsets.astype(jnp.int32))
    return best

def sunlight(facing, sun_tan, horizon):
    count = sun_tan.shape[0]
    angle = 2.0 * math.pi * jnp.arange(count, dtype=jnp.float32) / count
    elevation = jnp.arctan(sun_tan)
    sun_x = jnp.cos(elevation) * jnp.cos(angle)
    sun_y = jnp.cos(elevation) * jnp.sin(angle)
    sun_z = jnp.sin(elevation)
    incidence = sun_x[:, None] * facing[0][None, :] + sun_y[:, None] * facing[1][None, :] + sun_z[:, None] * facing[2][None, :]
    shade = jax.nn.sigmoid((sun_tan[:, None] - horizon) / shade_width)
    return solar_flux * jnp.maximum(incidence, 0.0) * shade

def conduct(soil, direct, bounce, albedo, conductivity):

    def advance(temps, inputs):
        light, scattered = inputs
        grad = temps[1:] - temps[:-1]
        edge = jnp.zeros((1, temps.shape[1]), jnp.float32)
        change = jnp.concatenate([grad, edge], 0) - jnp.concatenate([edge, grad], 0)
        temps = temps + conductivity[None, :] * change
        absorbed = (1.0 - albedo) * (light + scattered)
        top = temps[0] + surface_gain * (absorbed - emissivity * fourth(temps[0]))
        return (jnp.concatenate([top[None, :], temps[1:]], 0), None)
    final, unused = lax.scan(advance, soil, (direct, bounce))
    return final

def reference(positions, normals, area, albedo, conductivity, soil, sun_tan, samples, occupancy):
    horizon = lax.map(lambda offsets: profile_max(positions, offsets), samples)
    direct = sunlight(normals, sun_tan, horizon)
    radiance = (albedo[None, :] * direct + emissivity * fourth(soil[0])[None, :]).astype(jnp.bfloat16)
    table = occupancy.astype(jnp.float32)

    def per_block(block):
        start = (block * FAC).astype(jnp.int32)
        rec_pos = lax.dynamic_slice_in_dim(positions, start, FAC, 1)
        rec_nrm = lax.dynamic_slice_in_dim(normals, start, FAC, 1)
        weight = jnp.repeat(lax.dynamic_index_in_dim(table, block, 0, keepdims=False), FAC)[:, None]
        delta_x = positions[0][:, None] - rec_pos[0][None, :]
        delta_y = positions[1][:, None] - rec_pos[1][None, :]
        delta_z = positions[2][:, None] - rec_pos[2][None, :]
        facing = jnp.maximum(rec_nrm[0][None, :] * delta_x + rec_nrm[1][None, :] * delta_y + rec_nrm[2][None, :] * delta_z, 0.0)
        toward = jnp.maximum(-(normals[0][:, None] * delta_x + normals[1][:, None] * delta_y + normals[2][:, None] * delta_z), 0.0)
        spread = delta_x * delta_x + delta_y * delta_y + delta_z * delta_z + area[:, None]
        view = (facing * toward * area[:, None] * weight / (math.pi * spread * spread)).astype(jnp.bfloat16)
        return jnp.dot(radiance, view, preferred_element_type=jnp.float32)
    pieces = lax.map(per_block, jnp.arange(BLOCKS, dtype=jnp.int32))
    bounce = jnp.transpose(pieces, (1, 0, 2)).reshape(EPOCHS, F)
    final = conduct(soil, direct, bounce, albedo, conductivity)
    return (final, bounce)
```

```python
import functools
import math

import jax
import jax.numpy as jnp
from jax import lax
from jax.experimental import pallas as pl
from jax.experimental.pallas import tpu as pltpu
from jax.sharding import PartitionSpec as P

solar_flux = 2.0
emissivity = 0.9
surface_gain = 0.1
shade_width = 0.1
reach_offset = 0.05
GROUP = 8
CHUNK = 16


def fourth(value):
    square = value * value
    return square * square


def column(row, count):
    wide = jnp.broadcast_to(row[:, :count], (count, count))
    here = lax.broadcasted_iota(jnp.int32, (count, count), 0) == lax.broadcasted_iota(
        jnp.int32, (count, count), 1
    )
    return jnp.sum(jnp.where(here, wide, 0.0), axis=1, keepdims=True)


def kernel(
    n_recv,
    n_src,
    pos_ref,
    nrm_ref,
    area_ref,
    alb_ref,
    cond_ref,
    soil_ref,
    tan_ref,
    smp_ref,
    occ_ref,
    final_ref,
    bounce_ref,
    gath,
    planes,
    shifts,
    cols,
    view,
    direct_ref,
    radg,
    sems,
):
    n = n_recv * n_src
    width = pos_ref.shape[1]
    n_samples = smp_ref.shape[1]
    epochs = tan_ref.shape[1]
    layers = soil_ref.shape[0]
    bits = width.bit_length() - 1
    few = n <= 16
    me = lax.axis_index("recv") * n_src + lax.axis_index("src")

    def peer(k):
        p = lax.rem(me - k + n, n)
        return {"recv": p // n_src, "src": lax.rem(p, n_src)}

    def over(first, last, step):
        if few:
            for k in range(first, last):
                step(k)
        else:
            lax.fori_loop(first, last, lambda k, c: (step(k), c)[1], 0)

    barrier = pltpu.get_barrier_semaphore()
    over(
        1,
        n,
        lambda k: pl.semaphore_signal(
            barrier, inc=1, device_id=peer(k), device_id_type=pl.DeviceIdType.MESH
        ),
    )
    gath[0, 0:3, :] = pos_ref[...]
    gath[0, 3:6, :] = nrm_ref[...]
    gath[0, 6:7, :] = area_ref[...]
    gath[0, 7:8, 0:n_samples] = smp_ref[...].astype(jnp.float32)
    pl.semaphore_wait(barrier, n - 1)

    def send(ref, k, which):
        pltpu.make_async_remote_copy(
            src_ref=ref.at[0],
            dst_ref=ref.at[k],
            send_sem=sems.at[which],
            recv_sem=sems.at[which + 1],
            device_id=peer(k),
            device_id_type=pl.DeviceIdType.MESH,
        ).start()

    def everyone(ref, which):
        return pltpu.make_async_remote_copy(
            src_ref=ref.at[pl.ds(1, n - 1)],
            dst_ref=ref.at[pl.ds(1, n - 1)],
            send_sem=sems.at[which],
            recv_sem=sems.at[which + 1],
            device_id=peer(1),
            device_id_type=pl.DeviceIdType.MESH,
        )

    over(1, n, lambda k: send(gath, k, 0))

    mine = gath[0]
    tall = jnp.transpose(mine)
    for c in range(6):
        cols[c] = jnp.broadcast_to(tall[:, c : c + 1], (width, width))
    tan = column(tan_ref[...], epochs)
    angle = (
        2.0
        * math.pi
        * lax.broadcasted_iota(jnp.int32, (epochs, width), 0).astype(jnp.float32)
        / epochs
    )
    cos_e = 1.0 / jnp.sqrt(1.0 + tan * tan)
    incidence = (
        cos_e * jnp.cos(angle) * nrm_ref[0:1, :]
        + cos_e * jnp.sin(angle) * nrm_ref[1:2, :]
        + tan * cos_e * nrm_ref[2:3, :]
    )
    lit = solar_flux * jnp.maximum(incidence, 0.0)
    infrared = emissivity * fourth(soil_ref[0:1, :])

    everyone(gath, 0).wait_recv()
    for c in range(3):
        planes[c] = gath[:, c, :]
    rows = gath[:, 7, :]
    shifts[0:n, :] = rows
    shifts[n : 2 * n, :] = rows

    lane = lax.broadcasted_iota(jnp.int32, (GROUP, width), 1)
    px, py, pz = (jnp.broadcast_to(mine[c : c + 1, :], (GROUP, width)) for c in range(3))

    def azimuths(group):
        offset = n - me + group * GROUP
        steps = shifts[pl.ds(offset, GROUP), :].astype(jnp.int32)
        best = jnp.full((GROUP, width), -1e30, jnp.float32)
        for s in range(n_samples):
            shift = jnp.broadcast_to(steps[:, s : s + 1], (GROUP, width))
            row = ((shift + (width - 1) - lane) >> bits) & (n - 1)
            within = row & (GROUP - 1)
            part = row >> (GROUP.bit_length() - 1)
            turn = (lane + shift) & (width - 1)
            found = []
            for c in range(3):
                picked = None
                for g in range(n // GROUP):
                    block = planes[c, g * GROUP : (g + 1) * GROUP, :]
                    got = jnp.take_along_axis(block, within, axis=0)
                    picked = got if picked is None else jnp.where(part == g, got, picked)
                found.append(jnp.take_along_axis(picked, turn, axis=1))
            dx = found[0] - px
            dy = found[1] - py
            reach = jnp.sqrt(dx * dx + dy * dy) + reach_offset
            best = jnp.maximum(best, (found[2] - pz) / reach)
        start = group * GROUP
        direct_ref[pl.ds(start if few else pl.multiple_of(start, GROUP), GROUP), :] = best

    over(0, n // GROUP, azimuths)
    horizon = direct_ref[...]
    direct = lit * jax.nn.sigmoid((tan - horizon) / shade_width)
    direct_ref[...] = direct
    radg[0] = (alb_ref[...] * direct + infrared).astype(jnp.bfloat16)
    over(1, n, lambda k: send(radg, k, 2))

    def see(k, carry):
        block = gath[k]
        other = lax.rem(me + k, n)
        weight = occ_ref[me, other].astype(jnp.float32)
        sx, sy, sz, ox, oy, oz, size = (block[c : c + 1, :] for c in range(7))
        scale = size * weight / math.pi
        for i in range(width // CHUNK):
            at = slice(i * CHUNK, (i + 1) * CHUNK)
            dx = sx - cols[0, at, :]
            dy = sy - cols[1, at, :]
            dz = sz - cols[2, at, :]
            facing = cols[3, at, :] * dx + cols[4, at, :] * dy + cols[5, at, :] * dz
            toward = -(ox * dx + oy * dy + oz * dz)
            spread = dx * dx + dy * dy + dz * dz + size
            seen = jnp.maximum(facing, 0.0) * jnp.maximum(toward, 0.0) * scale
            view[k, at, :] = (seen / (spread * spread)).astype(jnp.bfloat16)
        return carry

    lax.fori_loop(0, n, see, 0)
    everyone(radg, 2).wait_recv()

    def fold(k, total):
        return total + lax.dot_general(
            radg[k], view[k], (((1,), (1,)), ((), ())), preferred_element_type=jnp.float32
        )

    total = jnp.zeros((epochs, width), jnp.float32)
    if few:
        for k in range(n):
            total = fold(k, total)
    else:
        total = lax.fori_loop(0, n, fold, total)
    bounce_ref[...] = total
    keep = surface_gain * (1.0 - alb_ref[...])
    direct_ref[...] = keep * (direct_ref[...] + total)
    cond = cond_ref[...]
    first = lax.broadcasted_iota(jnp.int32, (layers, width), 0) == 0
    last = lax.broadcasted_iota(jnp.int32, (layers, width), 0) == layers - 1

    def advance(t, temps):
        below = jnp.where(last, temps, pltpu.roll(temps, layers - 1, 0))
        above = jnp.where(first, temps, pltpu.roll(temps, 1, 0))
        temps = temps + cond * ((below - temps) - (temps - above))
        gain = direct_ref[pl.ds(t, 1), :] - (surface_gain * emissivity) * fourth(temps)
        return jnp.where(first, temps + gain, temps)

    temps = soil_ref[...]
    if few:
        for t in range(epochs):
            temps = advance(t, temps)
    else:
        temps = lax.fori_loop(0, epochs, advance, temps)
    final_ref[...] = temps
    everyone(gath, 0).wait_send()
    everyone(radg, 2).wait_send()


def body(positions, normals, area, albedo, conductivity, soil, sun_tan, samples, occupancy):
    n_recv = lax.axis_size("recv")
    n_src = lax.axis_size("src")
    n = n_recv * n_src
    width = positions.shape[1]
    epochs = sun_tan.shape[0]
    vmem = pl.BlockSpec(memory_space=pltpu.VMEM)
    return pl.pallas_call(
        functools.partial(kernel, n_recv, n_src),
        out_shape=(
            jax.ShapeDtypeStruct(soil.shape, jnp.float32),
            jax.ShapeDtypeStruct((epochs, width), jnp.float32),
        ),
        in_specs=[vmem] * 8 + [pl.BlockSpec(memory_space=pltpu.SMEM)],
        out_specs=(vmem, vmem),
        scratch_shapes=[
            pltpu.VMEM((n, 8, width), jnp.float32),
            pltpu.VMEM((3, n, width), jnp.float32),
            pltpu.VMEM((2 * n, width), jnp.float32),
            pltpu.VMEM((6, width, width), jnp.float32),
            pltpu.VMEM((n, width, width), jnp.bfloat16),
            pltpu.VMEM((epochs, width), jnp.float32),
            pltpu.VMEM((n, epochs, width), jnp.bfloat16),
            pltpu.SemaphoreType.DMA((4,)),
        ],
        compiler_params=pltpu.CompilerParams(collective_id=0, has_side_effects=True),
    )(
        positions,
        normals,
        area.reshape(1, width),
        albedo.reshape(1, width),
        conductivity.reshape(1, width),
        soil,
        sun_tan.reshape(1, epochs),
        samples,
        occupancy,
    )


def solution(mesh):
    in_specs = (
        P(None, ("basin", "recv", "src")),
        P(None, ("basin", "recv", "src")),
        P(("basin", "recv", "src")),
        P(("basin", "recv", "src")),
        P(("basin", "recv", "src")),
        P(None, ("basin", "recv", "src")),
        P(),
        P(("basin", "recv", "src"), None),
        P("basin", None),
    )
    out_specs = (P(None, ("basin", "recv", "src")), P(None, ("basin", "recv", "src")))
    return jax.shard_map(body, mesh=mesh, in_specs=in_specs, out_specs=out_specs, check_vma=False)
```

```python
import functools
import math

import jax
import jax.numpy as jnp
from jax import lax
from jax.experimental import pallas as pl
from jax.experimental.pallas import tpu as pltpu
from jax.sharding import PartitionSpec as P

solar_flux = 2.0
emissivity = 0.9
surface_gain = 0.1
shade_width = 0.1
reach_offset = 0.05
GROUP = 8
CHUNK = 16


def fourth(value):
    square = value * value
    return square * square


def column(row, count):
    wide = jnp.broadcast_to(row[:, :count], (count, count))
    here = lax.broadcasted_iota(jnp.int32, (count, count), 0) == lax.broadcasted_iota(
        jnp.int32, (count, count), 1
    )
    return jnp.sum(jnp.where(here, wide, 0.0), axis=1, keepdims=True)


def kernel(
    n_recv,
    n_src,
    pos_in,
    nrm_in,
    area_in,
    alb_in,
    cond_in,
    soil_in,
    tan_in,
    smp_in,
    occ_in,
    bounce_ref,
    heat_ref,
    cond_ref,
    soil_ref,
    pos_ref,
    nrm_ref,
    area_ref,
    alb_ref,
    tan_ref,
    smp_ref,
    occ_ref,
    near,
    far,
    planes,
    shifts,
    cols,
    view,
    direct_ref,
    radg,
    sems,
    loads,
):
    n = n_recv * n_src
    width = pos_ref.shape[1]
    n_samples = smp_ref.shape[1]
    epochs = tan_ref.shape[1]
    bits = width.bit_length() - 1
    few = n <= 16
    me = lax.axis_index("recv") * n_src + lax.axis_index("src")

    def peer(k):
        p = lax.rem(me - k + n, n)
        return {"recv": p // n_src, "src": lax.rem(p, n_src)}

    def over(first, last, step):
        if few:
            for k in sorted(range(first, last), key=lambda k: abs(2 * k - n)):
                step(k)
        else:
            lax.fori_loop(first, last, lambda k, c: (step(k), c)[1], 0)

    barrier = pltpu.get_barrier_semaphore()
    over(
        1,
        n,
        lambda k: pl.semaphore_signal(
            barrier, inc=1, device_id=peer(k), device_id_type=pl.DeviceIdType.MESH
        ),
    )
    pairs = (
        (pos_in, pos_ref),
        (smp_in, smp_ref),
        (nrm_in, nrm_ref),
        (area_in, area_ref),
        (tan_in, tan_ref),
        (soil_in, soil_ref),
        (alb_in, alb_ref),
        (cond_in, cond_ref),
        (occ_in.at[pl.ds(me, 1)], occ_ref),
    )
    fetched = [
        pltpu.make_async_copy(there, here, loads.at[i]) for i, (there, here) in enumerate(pairs)
    ]
    for copy in fetched:
        copy.start()
    for copy in fetched[:4]:
        copy.wait()
    near[0, 0:3, :] = pos_ref[...]
    near[0, 3:4, 0:n_samples] = smp_ref[...].astype(jnp.float32)
    far[0, 0:3, :] = nrm_ref[...]
    far[0, 3:4, :] = area_ref[...]
    for copy in fetched[4:]:
        copy.wait()
    pl.semaphore_wait(barrier, n - 1)

    def send(ref, k, which):
        pltpu.make_async_remote_copy(
            src_ref=ref.at[0],
            dst_ref=ref.at[k],
            send_sem=sems.at[which],
            recv_sem=sems.at[which + 1],
            device_id=peer(k),
            device_id_type=pl.DeviceIdType.MESH,
        ).start()

    def everyone(ref, which):
        return pltpu.make_async_remote_copy(
            src_ref=ref.at[pl.ds(1, n - 1)],
            dst_ref=ref.at[pl.ds(1, n - 1)],
            send_sem=sems.at[which],
            recv_sem=sems.at[which + 1],
            device_id=peer(1),
            device_id_type=pl.DeviceIdType.MESH,
        )

    over(1, n, lambda k: send(near, k, 0))
    over(1, n, lambda k: send(far, k, 4))

    mine = near[0]
    tall = jnp.transpose(jnp.concatenate([mine, far[0]], axis=0))
    for c, at in enumerate((0, 1, 2, 4, 5, 6)):
        cols[c] = jnp.broadcast_to(tall[:, at : at + 1], (width, width))
    tan = column(tan_ref[...], epochs)
    angle = (
        2.0
        * math.pi
        * lax.broadcasted_iota(jnp.int32, (epochs, width), 0).astype(jnp.float32)
        / epochs
    )
    cos_e = 1.0 / jnp.sqrt(1.0 + tan * tan)
    incidence = (
        cos_e * jnp.cos(angle) * nrm_ref[0:1, :]
        + cos_e * jnp.sin(angle) * nrm_ref[1:2, :]
        + tan * cos_e * nrm_ref[2:3, :]
    )
    lit = solar_flux * jnp.maximum(incidence, 0.0)
    infrared = emissivity * fourth(soil_ref[0:1, :])

    everyone(near, 0).wait_recv()
    for c in range(3):
        planes[c] = near[:, c, :]
    rows = near[:, 3, :]
    shifts[0:n, :] = rows
    shifts[n : 2 * n, :] = rows

    lane = lax.broadcasted_iota(jnp.int32, (GROUP, width), 1)
    px, py, pz = (jnp.broadcast_to(mine[c : c + 1, :], (GROUP, width)) for c in range(3))

    def azimuths(group):
        offset = n - me + group * GROUP
        steps = shifts[pl.ds(offset, GROUP), :].astype(jnp.int32)
        best = jnp.full((GROUP, width), -1e30, jnp.float32)
        for s in range(n_samples):
            shift = jnp.broadcast_to(steps[:, s : s + 1], (GROUP, width))
            row = ((shift + (width - 1) - lane) >> bits) & (n - 1)
            within = row & (GROUP - 1)
            part = row >> (GROUP.bit_length() - 1)
            turn = (lane + shift) & (width - 1)
            found = []
            for c in range(3):
                picked = None
                for g in range(n // GROUP):
                    block = planes[c, g * GROUP : (g + 1) * GROUP, :]
                    got = jnp.take_along_axis(block, within, axis=0)
                    picked = got if picked is None else jnp.where(part == g, got, picked)
                found.append(jnp.take_along_axis(picked, turn, axis=1))
            dx = found[0] - px
            dy = found[1] - py
            reach = jnp.sqrt(dx * dx + dy * dy) + reach_offset
            best = jnp.maximum(best, (found[2] - pz) / reach)
        start = group * GROUP
        direct_ref[pl.ds(start if few else pl.multiple_of(start, GROUP), GROUP), :] = best

    over(0, n // GROUP, azimuths)
    horizon = direct_ref[...]
    direct = lit * jax.nn.sigmoid((tan - horizon) / shade_width)
    direct_ref[...] = direct
    radg[0] = (alb_ref[...] * direct + infrared).astype(jnp.bfloat16)
    over(1, n, lambda k: send(radg, k, 2))

    def see(k, carry):
        weight = occ_ref[0, lax.rem(me + k, n)].astype(jnp.float32)
        sx, sy, sz = (near[k, c : c + 1, :] for c in range(3))
        ox, oy, oz, size = (far[k, c : c + 1, :] for c in range(4))
        scale = size * weight / math.pi
        for i in range(width // CHUNK):
            at = slice(i * CHUNK, (i + 1) * CHUNK)
            dx = sx - cols[0, at, :]
            dy = sy - cols[1, at, :]
            dz = sz - cols[2, at, :]
            facing = cols[3, at, :] * dx + cols[4, at, :] * dy + cols[5, at, :] * dz
            toward = -(ox * dx + oy * dy + oz * dz)
            spread = dx * dx + dy * dy + dz * dz + size
            seen = jnp.maximum(facing, 0.0) * jnp.maximum(toward, 0.0) * scale
            view[k, at, :] = (seen / (spread * spread)).astype(jnp.bfloat16)
        return carry

    everyone(far, 4).wait_recv()
    lax.fori_loop(0, n, see, 0)
    everyone(radg, 2).wait_recv()

    def fold(k, total):
        return total + lax.dot_general(
            radg[k], view[k], (((1,), (1,)), ((), ())), preferred_element_type=jnp.float32
        )

    total = jnp.zeros((epochs, width), jnp.float32)
    if few:
        for k in range(n):
            total = fold(k, total)
    else:
        total = lax.fori_loop(0, n, fold, total)
    bounce_ref[...] = total
    keep = surface_gain * (1.0 - alb_ref[...])
    heat_ref[...] = keep * (direct_ref[...] + total)
    everyone(near, 0).wait_send()
    everyone(far, 4).wait_send()
    everyone(radg, 2).wait_send()


def conduct(bounce_in, heat_ref, cond_ref, soil_ref, final_ref, bounce_ref):
    layers, width = soil_ref.shape
    epochs = heat_ref.shape[0]
    bounce_ref[...] = bounce_in[...]
    cond = cond_ref[...]
    first = lax.broadcasted_iota(jnp.int32, (layers, width), 0) == 0
    last = lax.broadcasted_iota(jnp.int32, (layers, width), 0) == layers - 1

    def advance(t, temps):
        below = jnp.where(last, temps, pltpu.roll(temps, layers - 1, 0))
        above = jnp.where(first, temps, pltpu.roll(temps, 1, 0))
        temps = temps + cond * ((below - temps) - (temps - above))
        gain = heat_ref[pl.ds(t, 1), :] - (surface_gain * emissivity) * fourth(temps)
        return jnp.where(first, temps + gain, temps)

    temps = soil_ref[...]
    if epochs <= 16:
        for t in range(epochs):
            temps = advance(t, temps)
    else:
        temps = lax.fori_loop(0, epochs, advance, temps)
    final_ref[...] = temps


def body(positions, normals, area, albedo, conductivity, soil, sun_tan, samples, occupancy):
    n_recv = lax.axis_size("recv")
    n_src = lax.axis_size("src")
    n = n_recv * n_src
    width = positions.shape[1]
    epochs = sun_tan.shape[0]
    vmem = pl.BlockSpec(memory_space=pltpu.VMEM)
    f32 = jnp.float32
    n_samples = samples.shape[1]
    held = pl.pallas_call(
        functools.partial(kernel, n_recv, n_src),
        out_shape=(
            pltpu.VMEM((epochs, width), f32),
            pltpu.VMEM((epochs, width), f32),
            pltpu.VMEM((1, width), f32),
            pltpu.VMEM(soil.shape, f32),
        ),
        in_specs=[pl.BlockSpec(memory_space=pl.ANY)] * 9,
        out_specs=(vmem,) * 4,
        scratch_shapes=[
            pltpu.VMEM((3, width), f32),
            pltpu.VMEM((3, width), f32),
            pltpu.VMEM((1, width), f32),
            pltpu.VMEM((1, width), f32),
            pltpu.VMEM((1, epochs), f32),
            pltpu.VMEM((1, n_samples), jnp.int32),
            pltpu.SMEM((1, occupancy.shape[1]), jnp.int32),
            pltpu.VMEM((n, 4, width), f32),
            pltpu.VMEM((n, 4, width), f32),
            pltpu.VMEM((3, n, width), f32),
            pltpu.VMEM((2 * n, width), f32),
            pltpu.VMEM((6, width, width), f32),
            pltpu.VMEM((n, width, width), jnp.bfloat16),
            pltpu.VMEM((epochs, width), f32),
            pltpu.VMEM((n, epochs, width), jnp.bfloat16),
            pltpu.SemaphoreType.DMA((6,)),
            pltpu.SemaphoreType.DMA((9,)),
        ],
        compiler_params=pltpu.CompilerParams(collective_id=0, has_side_effects=True),
    )(
        positions,
        normals,
        area.reshape(1, width),
        albedo.reshape(1, width),
        conductivity.reshape(1, width),
        soil,
        sun_tan.reshape(1, epochs),
        samples,
        occupancy,
    )
    return pl.pallas_call(
        conduct,
        out_shape=(
            jax.ShapeDtypeStruct(soil.shape, f32),
            jax.ShapeDtypeStruct((epochs, width), f32),
        ),
        in_specs=[vmem] * 4,
        out_specs=(vmem, vmem),
    )(*(pltpu.with_memory_space_constraint(value, pltpu.VMEM) for value in held))


def solution(mesh):
    in_specs = (
        P(None, ("basin", "recv", "src")),
        P(None, ("basin", "recv", "src")),
        P(("basin", "recv", "src")),
        P(("basin", "recv", "src")),
        P(("basin", "recv", "src")),
        P(None, ("basin", "recv", "src")),
        P(),
        P(("basin", "recv", "src"), None),
        P("basin", None),
    )
    out_specs = (P(None, ("basin", "recv", "src")), P(None, ("basin", "recv", "src")))
    return jax.shard_map(body, mesh=mesh, in_specs=in_specs, out_specs=out_specs, check_vma=False)
```

```python
import functools
import math

import jax
import jax.numpy as jnp
from jax import lax
from jax.experimental import pallas as pl
from jax.experimental.pallas import tpu as pltpu
from jax.sharding import PartitionSpec as P

solar_flux = 2.0
emissivity = 0.9
surface_gain = 0.1
shade_width = 0.1
reach_offset = 0.05
GROUP = 8
CHUNK = 16


def fourth(value):
    square = value * value
    return square * square


def column(row, count):
    wide = jnp.broadcast_to(row[:, :count], (count, count))
    here = lax.broadcasted_iota(jnp.int32, (count, count), 0) == lax.broadcasted_iota(
        jnp.int32, (count, count), 1
    )
    return jnp.sum(jnp.where(here, wide, 0.0), axis=1, keepdims=True)


def kernel(
    n_recv,
    n_src,
    pos_in,
    nrm_in,
    area_in,
    alb_in,
    cond_in,
    soil_in,
    tan_in,
    smp_in,
    occ_in,
    bounce_ref,
    heat_ref,
    cond_ref,
    soil_ref,
    pos_ref,
    nrm_ref,
    area_ref,
    alb_ref,
    tan_ref,
    smp_ref,
    occ_ref,
    near,
    far,
    planes,
    shifts,
    cols,
    view,
    direct_ref,
    lit_ref,
    tall_tan,
    radg,
    sems,
    loads,
):
    n = n_recv * n_src
    width = pos_ref.shape[1]
    n_samples = smp_ref.shape[1]
    epochs = tan_ref.shape[1]
    bits = width.bit_length() - 1
    few = n <= 16
    me = lax.axis_index("recv") * n_src + lax.axis_index("src")

    def peer(k):
        p = (me + (n - k)) & (n - 1)
        return {"recv": p >> (n_src.bit_length() - 1), "src": p & (n_src - 1)}

    def over(first, last, step):
        if few:
            for k in sorted(range(first, last), key=lambda k: abs(2 * k - n)):
                step(k)
        else:
            lax.fori_loop(first, last, lambda k, c: (step(k), c)[1], 0)

    barrier = pltpu.get_barrier_semaphore()
    over(
        1,
        n,
        lambda k: pl.semaphore_signal(
            barrier, inc=1, device_id=peer(k), device_id_type=pl.DeviceIdType.MESH
        ),
    )
    pairs = (
        (pos_in, pos_ref),
        (smp_in, smp_ref),
        (nrm_in, nrm_ref),
        (area_in, area_ref),
        (tan_in, tan_ref),
        (soil_in, soil_ref),
        (alb_in, alb_ref),
        (cond_in, cond_ref),
        (occ_in.at[pl.ds(me, 1)], occ_ref),
    )
    fetched = [
        pltpu.make_async_copy(there, here, loads.at[i]) for i, (there, here) in enumerate(pairs)
    ]
    for copy in fetched:
        copy.start()
    for copy in fetched[:4]:
        copy.wait()
    near[0, 0:3, :] = pos_ref[...]
    near[0, 3:4, 0:n_samples] = smp_ref[...].astype(jnp.float32)
    far[0, 0:3, :] = nrm_ref[...]
    far[0, 3:4, :] = area_ref[...]
    for copy in fetched[4:]:
        copy.wait()
    pl.semaphore_wait(barrier, n - 1)

    def send(ref, k, which):
        pltpu.make_async_remote_copy(
            src_ref=ref.at[0],
            dst_ref=ref.at[k],
            send_sem=sems.at[which],
            recv_sem=sems.at[which + 1],
            device_id=peer(k),
            device_id_type=pl.DeviceIdType.MESH,
        ).start()

    def everyone(ref, which):
        return pltpu.make_async_remote_copy(
            src_ref=ref.at[pl.ds(1, n - 1)],
            dst_ref=ref.at[pl.ds(1, n - 1)],
            send_sem=sems.at[which],
            recv_sem=sems.at[which + 1],
            device_id=peer(1),
            device_id_type=pl.DeviceIdType.MESH,
        )

    over(1, n, lambda k: send(near, k, 0))
    over(1, n, lambda k: send(far, k, 4))

    mine = near[0]
    tall = jnp.transpose(jnp.concatenate([mine, far[0]], axis=0))
    for c, at in enumerate((0, 1, 2, 4, 5, 6)):
        cols[c] = jnp.broadcast_to(tall[:, at : at + 1], (width, width))
    tan = column(tan_ref[...], epochs)
    angle = (
        2.0
        * math.pi
        * lax.broadcasted_iota(jnp.int32, (epochs, width), 0).astype(jnp.float32)
        / epochs
    )
    cos_e = 1.0 / jnp.sqrt(1.0 + tan * tan)
    incidence = (
        cos_e * jnp.cos(angle) * nrm_ref[0:1, :]
        + cos_e * jnp.sin(angle) * nrm_ref[1:2, :]
        + tan * cos_e * nrm_ref[2:3, :]
    )
    lit_ref[...] = solar_flux * jnp.maximum(incidence, 0.0)
    tall_tan[...] = jnp.broadcast_to(tan, (epochs, width))
    infrared = emissivity * fourth(soil_ref[0:1, :])

    everyone(near, 0).wait_recv()
    for c in range(3):
        planes[c] = near[:, c, :]
    rows = near[:, 3, :]
    shifts[0:n, :] = rows
    shifts[n : 2 * n, :] = rows

    lane = lax.broadcasted_iota(jnp.int32, (GROUP, width), 1)
    px, py, pz = (jnp.broadcast_to(mine[c : c + 1, :], (GROUP, width)) for c in range(3))

    def azimuths(group):
        offset = n - me + group * GROUP
        steps = shifts[pl.ds(offset, GROUP), :].astype(jnp.int32)
        best = jnp.full((GROUP, width), -1e30, jnp.float32)
        for s in range(n_samples):
            shift = jnp.broadcast_to(steps[:, s : s + 1], (GROUP, width))
            row = ((shift + (width - 1) - lane) >> bits) & (n - 1)
            within = row & (GROUP - 1)
            part = row >> (GROUP.bit_length() - 1)
            turn = (lane + shift) & (width - 1)
            found = []
            for c in range(3):
                picked = None
                for g in range(n // GROUP):
                    block = planes[c, g * GROUP : (g + 1) * GROUP, :]
                    got = jnp.take_along_axis(block, within, axis=0)
                    picked = got if picked is None else jnp.where(part == g, got, picked)
                found.append(jnp.take_along_axis(picked, turn, axis=1))
            dx = found[0] - px
            dy = found[1] - py
            reach = jnp.sqrt(dx * dx + dy * dy) + reach_offset
            best = jnp.maximum(best, (found[2] - pz) / reach)
        start = group * GROUP
        here = pl.ds(start if few else pl.multiple_of(start, GROUP), GROUP)
        direct = lit_ref[here, :] * jax.nn.sigmoid((tall_tan[here, :] - best) / shade_width)
        direct_ref[here, :] = direct
        radg[0, group] = (alb_ref[...] * direct + infrared).astype(jnp.bfloat16)
        over(1, n, lambda k: send(radg.at[:, group], k, 2))

    over(0, n // GROUP, azimuths)

    def see(k, carry):
        weight = occ_ref[0, lax.rem(me + k, n)].astype(jnp.float32)
        sx, sy, sz = (near[k, c : c + 1, :] for c in range(3))
        ox, oy, oz, size = (far[k, c : c + 1, :] for c in range(4))
        scale = size * weight / math.pi
        for i in range(width // CHUNK):
            at = slice(i * CHUNK, (i + 1) * CHUNK)
            dx = sx - cols[0, at, :]
            dy = sy - cols[1, at, :]
            dz = sz - cols[2, at, :]
            facing = cols[3, at, :] * dx + cols[4, at, :] * dy + cols[5, at, :] * dz
            toward = -(ox * dx + oy * dy + oz * dz)
            spread = dx * dx + dy * dy + dz * dz + size
            seen = jnp.maximum(facing, 0.0) * jnp.maximum(toward, 0.0) * scale
            view[k, at, :] = (seen / (spread * spread)).astype(jnp.bfloat16)
        return carry

    everyone(far, 4).wait_recv()
    lax.fori_loop(0, n, see, 0)
    everyone(radg, 2).wait_recv()

    def fold(k, total):
        sent = jnp.concatenate([radg[k, g] for g in range(epochs // GROUP)], axis=0)
        return total + lax.dot_general(
            sent, view[k], (((1,), (1,)), ((), ())), preferred_element_type=jnp.float32
        )

    total = jnp.zeros((epochs, width), jnp.float32)
    if few:
        for k in range(n):
            total = fold(k, total)
    else:
        total = lax.fori_loop(0, n, fold, total)
    bounce_ref[...] = total
    keep = surface_gain * (1.0 - alb_ref[...])
    heat_ref[...] = keep * (direct_ref[...] + total)
    everyone(near, 0).wait_send()
    everyone(far, 4).wait_send()
    everyone(radg, 2).wait_send()


def conduct(bounce_in, heat_ref, cond_ref, soil_ref, final_ref, bounce_ref):
    layers, width = soil_ref.shape
    epochs = heat_ref.shape[0]
    bounce_ref[...] = bounce_in[...]
    cond = cond_ref[...]
    first = lax.broadcasted_iota(jnp.int32, (layers, width), 0) == 0
    last = lax.broadcasted_iota(jnp.int32, (layers, width), 0) == layers - 1

    def advance(t, temps):
        below = jnp.where(last, temps, pltpu.roll(temps, layers - 1, 0))
        above = jnp.where(first, temps, pltpu.roll(temps, 1, 0))
        temps = temps + cond * ((below - temps) - (temps - above))
        gain = heat_ref[pl.ds(t, 1), :] - (surface_gain * emissivity) * fourth(temps)
        return jnp.where(first, temps + gain, temps)

    temps = soil_ref[...]
    if epochs <= 16:
        for t in range(epochs):
            temps = advance(t, temps)
    else:
        temps = lax.fori_loop(0, epochs, advance, temps)
    final_ref[...] = temps


def body(positions, normals, area, albedo, conductivity, soil, sun_tan, samples, occupancy):
    n_recv = lax.axis_size("recv")
    n_src = lax.axis_size("src")
    n = n_recv * n_src
    width = positions.shape[1]
    epochs = sun_tan.shape[0]
    vmem = pl.BlockSpec(memory_space=pltpu.VMEM)
    f32 = jnp.float32
    n_samples = samples.shape[1]
    held = pl.pallas_call(
        functools.partial(kernel, n_recv, n_src),
        out_shape=(
            pltpu.VMEM((epochs, width), f32),
            pltpu.VMEM((epochs, width), f32),
            pltpu.VMEM((1, width), f32),
            pltpu.VMEM(soil.shape, f32),
        ),
        in_specs=[pl.BlockSpec(memory_space=pl.ANY)] * 9,
        out_specs=(vmem,) * 4,
        scratch_shapes=[
            pltpu.VMEM((3, width), f32),
            pltpu.VMEM((3, width), f32),
            pltpu.VMEM((1, width), f32),
            pltpu.VMEM((1, width), f32),
            pltpu.VMEM((1, epochs), f32),
            pltpu.VMEM((1, n_samples), jnp.int32),
            pltpu.SMEM((1, occupancy.shape[1]), jnp.int32),
            pltpu.VMEM((n, 4, width), f32),
            pltpu.VMEM((n, 4, width), f32),
            pltpu.VMEM((3, n, width), f32),
            pltpu.VMEM((2 * n, width), f32),
            pltpu.VMEM((6, width, width), f32),
            pltpu.VMEM((n, width, width), jnp.bfloat16),
            pltpu.VMEM((epochs, width), f32),
            pltpu.VMEM((epochs, width), f32),
            pltpu.VMEM((epochs, width), f32),
            pltpu.VMEM((n, epochs // GROUP, GROUP, width), jnp.bfloat16),
            pltpu.SemaphoreType.DMA((6,)),
            pltpu.SemaphoreType.DMA((9,)),
        ],
        compiler_params=pltpu.CompilerParams(collective_id=0, has_side_effects=True),
    )(
        positions,
        normals,
        area.reshape(1, width),
        albedo.reshape(1, width),
        conductivity.reshape(1, width),
        soil,
        sun_tan.reshape(1, epochs),
        samples,
        occupancy,
    )
    return pl.pallas_call(
        conduct,
        out_shape=(
            jax.ShapeDtypeStruct(soil.shape, f32),
            jax.ShapeDtypeStruct((epochs, width), f32),
        ),
        in_specs=[vmem] * 4,
        out_specs=(vmem, vmem),
    )(*(pltpu.with_memory_space_constraint(value, pltpu.VMEM) for value in held))


def solution(mesh):
    in_specs = (
        P(None, ("basin", "recv", "src")),
        P(None, ("basin", "recv", "src")),
        P(("basin", "recv", "src")),
        P(("basin", "recv", "src")),
        P(("basin", "recv", "src")),
        P(None, ("basin", "recv", "src")),
        P(),
        P(("basin", "recv", "src"), None),
        P("basin", None),
    )
    out_specs = (P(None, ("basin", "recv", "src")), P(None, ("basin", "recv", "src")))
    return jax.shard_map(body, mesh=mesh, in_specs=in_specs, out_specs=out_specs, check_vma=False)
```
